128 devices in a mesh: dp: 16 (over z, y), ep: 8 (over x, core).
Axes of the slice: x: 4, y: 4, z: 4, core: 2. Of those that a mesh axis runs over, the one named last changes fastest.
Arguments:
- x_in: bfloat16 [32768, 4096], P(('dp', 'ep'))
- ln_gain: float32 [4096], replicated
- ln_bias: float32 [4096], replicated
- w_router: bfloat16 [4096, 16], replicated
- w_gate: bfloat16 [16, 4096, 448], P('ep')
- w_up: bfloat16 [16, 4096, 448], P('ep')
- w_down: bfloat16 [16, 448, 4096], P('ep')
- expert_ids: int32 [32768, 2], P(('dp', 'ep'))
- slot_ids: int32 [32768, 2], P(('dp', 'ep'))
- d_out: bfloat16 [32768, 4096], P(('dp', 'ep'))
Outputs:
- output 1: bfloat16 [32768, 4096], P(('dp', 'ep'))
- output 2: bfloat16 [32768, 4096], P(('dp', 'ep'))
- output 3: float32 [4096], replicated
- output 4: float32 [4096], replicated
- output 5: float32 [4096, 16], replicated
- output 6: float32 [16, 4096, 448], P('ep')
- output 7: float32 [16, 4096, 448], P('ep')
- output 8: float32 [16, 448, 4096], P('ep')
All inputs are finite; a program needn't handle non-finite values.
Results may differ from the reference program's by a relative error of at most 0.00533895.
Values are sent between devices in bfloat16 or wider.
A program may use at most 1 GiB of HBM per device.

```python
import jax
import jax.numpy as jnp
from jax import lax

D = 4096
FF = 448
EXPERTS = 16
TOP = 2
TOKENS_DEV = 256
DEVICES = 128
CAPACITY = 40
TOKENS = DEVICES * TOKENS_DEV
SLOT_ROWS = EXPERTS * CAPACITY
LN_EPS = 1e-5


def draw_routing(key_route):
    key_hot, key_perm, key_first, key_shift = jax.random.split(key_route, 4)
    hot_expert = jax.random.randint(key_hot, (DEVICES, 1), 0, EXPERTS)
    perm_keys = jax.random.split(key_perm, DEVICES)
    perm_pos = jax.vmap(lambda key_one: jax.random.permutation(key_one, TOKENS_DEV))(perm_keys)
    forced = perm_pos < (3 * CAPACITY) // 2
    first_pick = jax.random.randint(key_first, (DEVICES, TOKENS_DEV), 0, EXPERTS)
    first_pick = jnp.where(forced, hot_expert, first_pick)
    shift_by = jax.random.randint(key_shift, (DEVICES, TOKENS_DEV), 1, EXPERTS)
    second_pick = (first_pick + shift_by) % EXPERTS
    choice = jnp.stack([first_pick, second_pick], axis=-1)
    flat_pick = choice.reshape(DEVICES, TOKENS_DEV * TOP)
    onehot = (flat_pick[:, :, None] == jnp.arange(EXPERTS)[None, None, :]).astype(jnp.int32)
    before = jnp.cumsum(onehot, axis=1) - onehot
    pair_rank = jnp.sum(before * onehot, axis=-1)
    slot_pos = jnp.where(pair_rank < CAPACITY, pair_rank, -1)
    return choice.reshape(TOKENS, TOP).astype(jnp.int32), slot_pos.reshape(TOKENS, TOP).astype(jnp.int32)


def setup_inputs(seed: int = 0) -> dict:
    key_root = jax.random.key(seed)
    key_list = jax.random.split(key_root, 10)
    x_in = jax.random.normal(key_list[0], (TOKENS, D), jnp.float32).astype(jnp.bfloat16)
    ln_gain = 1.0 + 0.3 * jax.random.normal(key_list[1], (D,), jnp.float32)
    ln_bias = 0.3 * jax.random.normal(key_list[2], (D,), jnp.float32)
    w_router = (jax.random.normal(key_list[3], (D, EXPERTS), jnp.float32) * D ** -0.5).astype(jnp.bfloat16)
    w_gate = (jax.random.normal(key_list[4], (EXPERTS, D, FF), jnp.float32) * D ** -0.5).astype(jnp.bfloat16)
    w_up = (jax.random.normal(key_list[5], (EXPERTS, D, FF), jnp.float32) * D ** -0.5).astype(jnp.bfloat16)
    w_down = (jax.random.normal(key_list[6], (EXPERTS, FF, D), jnp.float32) * (2.0 * FF ** -0.5)).astype(jnp.bfloat16)
    expert_ids, slot_ids = draw_routing(key_list[7])
    d_out = jax.random.normal(key_list[8], (TOKENS, D), jnp.float32).astype(jnp.bfloat16)
    return {"x_in": x_in, "ln_gain": ln_gain, "ln_bias": ln_bias, "w_router": w_router, "w_gate": w_gate, "w_up": w_up, "w_down": w_down, "expert_ids": expert_ids, "slot_ids": slot_ids, "d_out": d_out}


def to_bf16_grid(array_in):
    return array_in.astype(jnp.bfloat16).astype(jnp.float32)


def reference(x_in, ln_gain, ln_bias, w_router, w_gate, w_up, w_down, expert_ids, slot_ids, d_out):
    ids_dev = expert_ids.reshape(DEVICES, TOKENS_DEV, TOP)
    slots_dev = slot_ids.reshape(DEVICES, TOKENS_DEV, TOP)
    target = jnp.where(slots_dev >= 0, ids_dev * CAPACITY + slots_dev, -1)
    pair_hot = (target[..., None] == jnp.arange(SLOT_ROWS)).astype(jnp.float32)
    token_hot = jnp.sum(pair_hot, axis=2)

    def block_fn(x_f, gain_vec, bias_vec, router_f, gate_f, up_f, down_f):
        x_dev = x_f.reshape(DEVICES, TOKENS_DEV, D)
        mean_x = jnp.mean(x_dev, axis=-1, keepdims=True)
        centered = x_dev - mean_x
        var_x = jnp.mean(centered * centered, axis=-1, keepdims=True)
        normed = centered * lax.rsqrt(var_x + LN_EPS)
        hidden = to_bf16_grid(normed * gain_vec + bias_vec)
        logits = jnp.einsum("dtm,me->dte", hidden, router_f)
        gate_probs = jax.nn.softmax(jnp.take_along_axis(logits, ids_dev, axis=-1), axis=-1)
        buffers = to_bf16_grid(jnp.einsum("dts,dtm->dsm", token_hot, hidden))
        buffers = buffers.reshape(DEVICES, EXPERTS, CAPACITY, D)
        act_gate = to_bf16_grid(jnp.einsum("decm,emf->decf", buffers, gate_f))
        act_up = to_bf16_grid(jnp.einsum("decm,emf->decf", buffers, up_f))
        act_mix = to_bf16_grid(jax.nn.silu(act_gate) * act_up)
        expert_out = to_bf16_grid(jnp.einsum("decf,efm->decm", act_mix, down_f))
        pair_out = jnp.einsum("dtks,dsm->dtkm", pair_hot, expert_out.reshape(DEVICES, SLOT_ROWS, D))
        mixed = jnp.einsum("dtk,dtkm->dtm", gate_probs, pair_out)
        return to_bf16_grid(x_dev + mixed).reshape(TOKENS, D)

    moe_f, pullback = jax.vjp(block_fn, x_in.astype(jnp.float32), ln_gain, ln_bias, w_router.astype(jnp.float32), w_gate.astype(jnp.float32), w_up.astype(jnp.float32), w_down.astype(jnp.float32))
    grad_list = pullback(d_out.astype(jnp.float32))
    return (moe_f.astype(jnp.bfloat16), grad_list[0].astype(jnp.bfloat16), grad_list[1], grad_list[2], grad_list[3], grad_list[4], grad_list[5], grad_list[6])
```

```python
import jax
import jax.numpy as jnp
from jax import lax
from jax.experimental import pallas as pl
from jax.sharding import Mesh, PartitionSpec as P

LN_EPS = 1e-5
BF = jnp.bfloat16
F32 = jnp.float32
NZ = NY = NX = 4
NC = 2
AXES = ("z", "y", "x", "c")


def capacity_for(tokens_dev, experts, n_top):
    return 8 * ((5 * tokens_dev * n_top + 32 * experts - 1) // (32 * experts))


def norm_forward(x_loc, ln_gain, ln_bias):
    x_f = x_loc.astype(F32)
    mean_x = jnp.mean(x_f, axis=-1, keepdims=True)
    centered = x_f - mean_x
    var_x = jnp.mean(centered * centered, axis=-1, keepdims=True)
    inv_std = lax.rsqrt(var_x + LN_EPS)
    normed = centered * inv_std
    hidden = (normed * ln_gain + ln_bias).astype(BF)
    return x_f, hidden, normed, inv_std


def norm_backward(d_hidden, normed, inv_std, ln_gain):
    d_normed = d_hidden * ln_gain
    mean_dn = jnp.mean(d_normed, axis=-1, keepdims=True)
    mean_dnn = jnp.mean(d_normed * normed, axis=-1, keepdims=True)
    return inv_std * (d_normed - mean_dn - normed * mean_dnn)


def router_forward(hidden, w_router, ids_loc):
    experts = w_router.shape[1]
    logits = jnp.dot(hidden, w_router, preferred_element_type=F32)
    pick_mask = (ids_loc[..., None] == jnp.arange(experts)).astype(F32)
    chosen = jnp.sum(pick_mask * logits[..., None, :], axis=-1)
    return jax.nn.softmax(chosen, axis=-1), pick_mask


def router_backward(gate_probs, pick_mask, pair_out, dout_f):
    d_gates = jnp.sum(pair_out * dout_f[:, None, :], axis=-1)
    d_chosen = gate_probs * (d_gates - jnp.sum(gate_probs * d_gates, axis=-1, keepdims=True))
    return jnp.sum(d_chosen[..., None] * pick_mask, axis=-2)


def home_of(expert):
    x, local = expert // 4, expert % 4
    y = (local >> 1) | ((local & 1) << 1)
    return y * NX + x


def weights_here(w_loc):
    y, c = lax.axis_index("y"), lax.axis_index("c")
    mine = lax.dynamic_index_in_dim(w_loc, y >> 1, 0, keepdims=False)
    pairs = [(yy * NC + (yy & 1), yy * NC + 1 - (yy & 1)) for yy in range(NY)]
    other = lax.ppermute(mine, ("y", "c"), pairs)
    return jnp.where(c == (y & 1), mine, other)


def to_owner_core(grad):
    pairs = []
    for yy in range(NY):
        own = yy & 1
        pairs.append((yy * NC + own, yy * NC + own))
        pairs.append((yy * NC + 1 - own, (yy ^ 1) * NC + own))
    return lax.ppermute(grad, ("y", "c"), pairs)


def dispatch(rows):
    return lax.all_to_all(rows, ("y", "x"), 0, 0, tiled=True)


def reduce_grad(factor_pair, rows):
    c = lax.axis_index("c")
    first, second = factor_pair
    away = jnp.where(c == 0, second, first)
    here = jnp.where(c == 0, first, second)
    partial = jnp.einsum("rf,rm->fm", away, rows, preferred_element_type=F32)
    sent = lax.ppermute(partial, "c", [(0, 1), (1, 0)])
    pair = jnp.einsum("rf,rm->fm", here, rows, preferred_element_type=F32) + sent
    return lax.psum_scatter(pair, "z", scatter_dimension=0, tiled=True)


def copy_out(array):
    n, rows, d = array.shape
    step = rows // 4

    def body(src_ref, dst_ref):
        dst_ref[...] = src_ref[...]

    return pl.pallas_call(
        body,
        grid=(n, 4),
        in_specs=[pl.BlockSpec((1, step, d), lambda i, k: (i, k, 0))],
        out_specs=pl.BlockSpec((1, step, d), lambda i, k: (i, k, 0)),
        out_shape=jax.ShapeDtypeStruct(array.shape, array.dtype),
        cost_estimate=pl.CostEstimate(flops=5000000000, bytes_accessed=8 * n * rows * d, transcendentals=0),
    )(array)


def gather_grad(grad):
    full = lax.all_gather(grad, ("y", "z"), axis=0, tiled=True)
    return full.reshape(2, full.shape[0] // 2, full.shape[1])


def small_psum(parts):
    stacked = jnp.concatenate(parts, axis=0)
    rows, d = stacked.shape
    n = NX * NC
    cut = jnp.swapaxes(stacked.reshape(rows, n, d // n), 0, 1)
    got = lax.all_to_all(cut, ("x", "c"), 0, 0, tiled=True)
    part = jnp.sum(got, axis=0)
    part = jnp.sum(lax.all_gather(part, ("z", "y"), axis=0, tiled=False), axis=0)
    full = lax.all_gather(part, ("x", "c"), axis=0, tiled=False)
    return jnp.swapaxes(full, 0, 1).reshape(rows, d)


def solution(mesh):
    inner = Mesh(mesh.devices.reshape(NZ, NY, NX, NC), AXES)
    tok_spec = P(AXES, None)
    exp_spec = P(("x", "c"), None, None)

    def local_step(x_loc, ln_gain, ln_bias, w_router, gate_loc, up_loc, down_loc, ids_loc, slots_loc, dout_loc):
        tokens_dev, model_dim = x_loc.shape
        experts = w_router.shape[1]
        n_top = ids_loc.shape[1]
        capacity = capacity_for(tokens_dev, experts, n_top)
        slots = experts * capacity
        w_gate = weights_here(gate_loc)
        w_up = weights_here(up_loc)
        w_down = weights_here(down_loc)
        x_f, hidden, normed, inv_std = norm_forward(x_loc, ln_gain, ln_bias)
        gate_probs, pick_mask = router_forward(hidden, w_router, ids_loc)
        target = jnp.where(slots_loc >= 0, home_of(ids_loc) * capacity + slots_loc, -1)
        pair_hot = (target[..., None] == jnp.arange(slots)).astype(BF)
        token_hot = jnp.sum(pair_hot, axis=1)
        send_rows = jnp.einsum("ts,tm->sm", token_hot, hidden, preferred_element_type=F32).astype(BF)
        expert_in = dispatch(send_rows)
        send_rows, dout_late = lax.optimization_barrier((send_rows, dout_loc))
        dout_f = dout_late.astype(F32)
        pair_grad = (gate_probs[..., None] * dout_f[:, None, :]).astype(BF)
        send_grad = jnp.einsum("tks,tkm->sm", pair_hot, pair_grad, preferred_element_type=F32).astype(BF)
        grad_in = dispatch(send_grad)

        pre_gate = jnp.dot(expert_in, w_gate, preferred_element_type=F32).astype(BF)
        pre_up = jnp.dot(expert_in, w_up, preferred_element_type=F32).astype(BF)
        gate_f = pre_gate.astype(F32)
        up_f = pre_up.astype(F32)
        sig_gate = jax.nn.sigmoid(gate_f)
        act_mix = (gate_f * sig_gate * up_f).astype(BF)
        expert_out = jnp.dot(act_mix, w_down, preferred_element_type=F32).astype(BF)

        expert_out, grad_in = lax.optimization_barrier((expert_out, grad_in))
        d_mix = jnp.einsum("rm,fm->rf", grad_in, w_down, preferred_element_type=F32).astype(BF).astype(F32)
        d_pre_gate = (d_mix * up_f * sig_gate * (1.0 + gate_f * (1.0 - sig_gate))).astype(BF)
        d_pre_up = (d_mix * gate_f * sig_gate).astype(BF)

        ff = act_mix.shape[1]
        ret_rows = dispatch(expert_out)
        grad_down = reduce_grad((act_mix[:, : ff // 2], act_mix[:, ff // 2 :]), grad_in)
        grad_gate_up = reduce_grad((d_pre_gate, d_pre_up), expert_in)
        d_expert_in = (jnp.einsum("rf,mf->rm", d_pre_gate, w_gate, preferred_element_type=F32) + jnp.einsum("rf,mf->rm", d_pre_up, w_up, preferred_element_type=F32)).astype(BF)
        ret_rows, d_expert_in = lax.optimization_barrier((ret_rows, d_expert_in))
        d_rows = dispatch(d_expert_in)
        grad_down = to_owner_core(grad_down)
        grad_down, grad_gate_up, d_rows = lax.optimization_barrier((grad_down, grad_gate_up, d_rows))
        full_down = copy_out(gather_grad(grad_down))
        gate_up = gather_grad(to_owner_core(grad_gate_up))
        full_gate = jnp.swapaxes(gate_up[:, :ff], 1, 2)
        full_up = jnp.swapaxes(gate_up[:, ff:], 1, 2)

        pair_out = jnp.dot(pair_hot.reshape(tokens_dev * n_top, slots), ret_rows, preferred_element_type=F32).reshape(tokens_dev, n_top, model_dim)
        mixed = jnp.sum(gate_probs[..., None] * pair_out, axis=1)
        moe_out = (x_f + mixed).astype(BF)
        d_logits = router_backward(gate_probs, pick_mask, pair_out, dout_f)
        d_hidden_moe = jnp.einsum("ts,sm->tm", token_hot, d_rows, preferred_element_type=F32)
        d_hidden_router = jnp.einsum("te,me->tm", d_logits, w_router, preferred_element_type=F32)
        d_hidden = (d_hidden_moe + d_hidden_router).astype(BF).astype(F32)
        grad_x = (dout_f + norm_backward(d_hidden, normed, inv_std, ln_gain)).astype(BF)
        small = small_psum([jnp.einsum("te,tm->em", d_logits, hidden, preferred_element_type=F32), jnp.sum(d_hidden * normed, axis=0)[None], jnp.sum(d_hidden, axis=0)[None]])
        return (moe_out, grad_x, small[experts], small[experts + 1], small[:experts].T, full_gate, full_up, full_down)

    return jax.shard_map(local_step, mesh=inner, in_specs=(tok_spec, P(None), P(None), P(None, None), exp_spec, exp_spec, exp_spec, tok_spec, tok_spec, tok_spec), out_specs=(tok_spec, tok_spec, P(None), P(None), P(None, None), exp_spec, exp_spec, exp_spec), check_vma=False)
```

```python
import jax
import jax.numpy as jnp
from jax import lax
from jax.experimental import pallas as pl
from jax.experimental.pallas import tpu as pltpu
from jax.sharding import Mesh, PartitionSpec as P

LN_EPS = 1e-5
BF = jnp.bfloat16
F32 = jnp.float32
NZ = NY = NX = 4
NC = 2
AXES = ("z", "y", "x", "c")


def capacity_for(tokens_dev, experts, n_top):
    return 8 * ((5 * tokens_dev * n_top + 32 * experts - 1) // (32 * experts))


def norm_forward(x_loc, ln_gain, ln_bias):
    x_f = x_loc.astype(F32)
    mean_x = jnp.mean(x_f, axis=-1, keepdims=True)
    centered = x_f - mean_x
    var_x = jnp.mean(centered * centered, axis=-1, keepdims=True)
    inv_std = lax.rsqrt(var_x + LN_EPS)
    normed = centered * inv_std
    hidden = (normed * ln_gain + ln_bias).astype(BF)
    return x_f, hidden, normed, inv_std


def norm_backward(d_hidden, normed, inv_std, ln_gain):
    d_normed = d_hidden * ln_gain
    mean_dn = jnp.mean(d_normed, axis=-1, keepdims=True)
    mean_dnn = jnp.mean(d_normed * normed, axis=-1, keepdims=True)
    return inv_std * (d_normed - mean_dn - normed * mean_dnn)


def router_forward(hidden, w_router, ids_loc):
    experts = w_router.shape[1]
    logits = jnp.dot(hidden, w_router, preferred_element_type=F32)
    pick_mask = (ids_loc[..., None] == jnp.arange(experts)).astype(F32)
    chosen = jnp.sum(pick_mask * logits[..., None, :], axis=-1)
    return jax.nn.softmax(chosen, axis=-1), pick_mask


def router_backward(gate_probs, pick_mask, pair_out, dout_f):
    d_gates = jnp.sum(pair_out * dout_f[:, None, :], axis=-1)
    d_chosen = gate_probs * (d_gates - jnp.sum(gate_probs * d_gates, axis=-1, keepdims=True))
    return jnp.sum(d_chosen[..., None] * pick_mask, axis=-2)


def home_of(expert):
    x, local = expert // 4, expert % 4
    y = (local >> 1) | ((local & 1) << 1)
    return y * NX + x


def weights_here(w_loc):
    y, c = lax.axis_index("y"), lax.axis_index("c")
    mine = lax.dynamic_index_in_dim(w_loc, y >> 1, 0, keepdims=False)
    pairs = [(yy * NC + (yy & 1), yy * NC + 1 - (yy & 1)) for yy in range(NY)]
    other = lax.ppermute(mine, ("y", "c"), pairs)
    return jnp.where(c == (y & 1), mine, other)


CUT = 512
CHUNK = 32
ROWS = 160
NT = (((1,), (1,)), ((), ()))
NN = (((1,), (0,)), ((), ()))


def dot(a, b, dims):
    return lax.dot_general(a, b, dims, preferred_element_type=F32)


def cost_of(products, rows, ff, d):
    return pl.CostEstimate(flops=2 * products * rows * ff * d, bytes_accessed=2 * (rows + products * ff) * d, transcendentals=0)


def gate_and_up(rows_in, gate_t, up_t):
    rows, d = rows_in.shape
    ff = gate_t.shape[0]
    last = d // CUT - 1

    def body(x_ref, wg_ref, wu_ref, a_ref, u_ref, m_ref, acc_g, acc_u):
        @pl.when(pl.program_id(0) == 0)
        def _():
            acc_g[...] = jnp.zeros_like(acc_g)
            acc_u[...] = jnp.zeros_like(acc_u)

        @pl.loop(0, rows // ROWS)
        def _(i):
            at = pl.ds(i * ROWS, ROWS)
            acc_g[at, :] += dot(x_ref[at, :], wg_ref[...], NT)
            acc_u[at, :] += dot(x_ref[at, :], wu_ref[...], NT)

        @pl.when(pl.program_id(0) == last)
        def _():
            @pl.loop(0, rows // CHUNK)
            def _(i):
                at = pl.ds(i * CHUNK, CHUNK)
                a = acc_g[at, :].astype(BF)
                u = acc_u[at, :].astype(BF)
                a_f = a.astype(F32)
                a_ref[at, :] = a
                u_ref[at, :] = u
                m_ref[at, :] = (a_f * jax.nn.sigmoid(a_f) * u.astype(F32)).astype(BF)

    out = jax.ShapeDtypeStruct((rows, ff), BF)
    whole = pl.BlockSpec((rows, ff), lambda k: (0, 0))
    weight = pl.BlockSpec((ff, CUT), lambda k: (0, k))
    return pl.pallas_call(
        body,
        grid=(d // CUT,),
        in_specs=[pl.BlockSpec((rows, CUT), lambda k: (0, k)), weight, weight],
        out_specs=[whole, whole, whole],
        out_shape=[out, out, out],
        scratch_shapes=[pltpu.VMEM((rows, ff), F32), pltpu.VMEM((rows, ff), F32)],
        cost_estimate=cost_of(2, rows, ff, d),
    )(rows_in, gate_t, up_t)


def gate_and_up_backward(grad_in, down, pre_gate, pre_up):
    rows, d = grad_in.shape
    ff = down.shape[0]
    last = d // CUT - 1

    def body(g_ref, w_ref, a_ref, u_ref, da_ref, du_ref, acc):
        @pl.when(pl.program_id(0) == 0)
        def _():
            acc[...] = jnp.zeros_like(acc)

        @pl.loop(0, 2)
        def _(i):
            at = pl.ds(i * (rows // 2), rows // 2)
            acc[at, :] += dot(g_ref[at, :], w_ref[...], NT)

        @pl.when(pl.program_id(0) == last)
        def _():
            @pl.loop(0, rows // CHUNK)
            def _(i):
                at = pl.ds(i * CHUNK, CHUNK)
                dm = acc[at, :].astype(BF).astype(F32)
                a = a_ref[at, :].astype(F32)
                u = u_ref[at, :].astype(F32)
                sig = jax.nn.sigmoid(a)
                da_ref[at, :] = (dm * u * sig * (1.0 + a * (1.0 - sig))).astype(BF)
                du_ref[at, :] = (dm * a * sig).astype(BF)

    out = jax.ShapeDtypeStruct((rows, ff), BF)
    whole = pl.BlockSpec((rows, ff), lambda k: (0, 0))
    return pl.pallas_call(
        body,
        grid=(d // CUT,),
        in_specs=[pl.BlockSpec((rows, CUT), lambda k: (0, k)), pl.BlockSpec((ff, CUT), lambda k: (0, k)), whole, whole],
        out_specs=[whole, whole],
        out_shape=[out, out],
        scratch_shapes=[pltpu.VMEM((rows, ff), F32)],
        cost_estimate=cost_of(1, rows, ff, d),
    )(grad_in, down, pre_gate, pre_up)


def rows_from(factors, weights):
    rows, ff = factors[0].shape
    d = weights[0].shape[1]
    n = len(factors)

    def body(*refs):
        out_ref = refs[-1]

        @pl.loop(0, rows // ROWS)
        def _(i):
            at = pl.ds(i * ROWS, ROWS)
            total = dot(refs[0][at, :], refs[n][...], NN)
            for j in range(1, n):
                total += dot(refs[j][at, :], refs[n + j][...], NN)
            out_ref[at, :] = total.astype(BF)

    return pl.pallas_call(
        body,
        grid=(d // CUT,),
        in_specs=[pl.BlockSpec((rows, ff), lambda k: (0, 0))] * n + [pl.BlockSpec((ff, CUT), lambda k: (0, k))] * n,
        out_specs=pl.BlockSpec((rows, CUT), lambda k: (0, k)),
        out_shape=jax.ShapeDtypeStruct((rows, d), BF),
        cost_estimate=cost_of(n, rows, ff, d),
    )(*factors, *weights)


def to_owner_core(grad):
    pairs = []
    for yy in range(NY):
        own = yy & 1
        pairs.append((yy * NC + own, yy * NC + own))
        pairs.append((yy * NC + 1 - own, (yy ^ 1) * NC + own))
    return lax.ppermute(grad, ("y", "c"), pairs)


def dispatch(rows):
    return lax.all_to_all(rows, ("y", "x"), 0, 0, tiled=True)


def reduce_grad(factor_pair, rows):
    c = lax.axis_index("c")
    first, second = factor_pair
    away = jnp.where(c == 0, second, first)
    here = jnp.where(c == 0, first, second)
    partial = jnp.einsum("rf,rm->fm", away, rows, preferred_element_type=F32)
    sent = lax.ppermute(partial, "c", [(0, 1), (1, 0)])
    pair = jnp.einsum("rf,rm->fm", here, rows, preferred_element_type=F32) + sent
    return lax.psum_scatter(pair, "z", scatter_dimension=0, tiled=True)


def copy_out(array):
    n, rows, d = array.shape
    step = rows // 4

    def body(src_ref, dst_ref):
        @pl.loop(0, step // 8)
        def _(i):
            at = pl.ds(i * 8, 8)
            dst_ref[0, at, :] = src_ref[0, at, :]

    return pl.pallas_call(
        body,
        grid=(n, 4),
        in_specs=[pl.BlockSpec((1, step, d), lambda i, k: (i, k, 0))],
        out_specs=pl.BlockSpec((1, step, d), lambda i, k: (i, k, 0)),
        out_shape=jax.ShapeDtypeStruct(array.shape, array.dtype),
        cost_estimate=pl.CostEstimate(flops=5000000000, bytes_accessed=8 * n * rows * d, transcendentals=0),
    )(array)


def gather_grad(grad):
    full = lax.all_gather(grad, ("y", "z"), axis=0, tiled=True)
    return full.reshape(2, full.shape[0] // 2, full.shape[1])


def small_psum(parts):
    stacked = jnp.concatenate(parts, axis=0)
    rows, d = stacked.shape
    n = NX * NC
    cut = jnp.swapaxes(stacked.reshape(rows, n, d // n), 0, 1)
    got = lax.all_to_all(cut, ("x", "c"), 0, 0, tiled=True)
    part = jnp.sum(got, axis=0)
    part = jnp.sum(lax.all_gather(part, ("z", "y"), axis=0, tiled=False), axis=0)
    full = lax.all_gather(part, ("x", "c"), axis=0, tiled=False)
    return jnp.swapaxes(full, 0, 1).reshape(rows, d)


def solution(mesh):
    inner = Mesh(mesh.devices.reshape(NZ, NY, NX, NC), AXES)
    tok_spec = P(AXES, None)
    exp_spec = P(("x", "c"), None, None)

    def local_step(x_loc, ln_gain, ln_bias, w_router, gate_loc, up_loc, down_loc, ids_loc, slots_loc, dout_loc):
        tokens_dev, model_dim = x_loc.shape
        experts = w_router.shape[1]
        n_top = ids_loc.shape[1]
        capacity = capacity_for(tokens_dev, experts, n_top)
        slots = experts * capacity
        w_gate = weights_here(jnp.swapaxes(gate_loc, 1, 2))
        w_up = weights_here(jnp.swapaxes(up_loc, 1, 2))
        w_down = weights_here(down_loc)
        x_f, hidden, normed, inv_std = norm_forward(x_loc, ln_gain, ln_bias)
        gate_probs, pick_mask = router_forward(hidden, w_router, ids_loc)
        target = jnp.where(slots_loc >= 0, home_of(ids_loc) * capacity + slots_loc, -1)
        pair_hot = (target[..., None] == jnp.arange(slots)).astype(BF)
        token_hot = jnp.sum(pair_hot, axis=1)
        send_rows = jnp.einsum("ts,tm->sm", token_hot, hidden, preferred_element_type=F32).astype(BF)
        expert_in = dispatch(send_rows)
        send_rows, dout_late = lax.optimization_barrier((send_rows, dout_loc))
        dout_f = dout_late.astype(F32)
        pair_grad = (gate_probs[..., None] * dout_f[:, None, :]).astype(BF)
        send_grad = jnp.einsum("tks,tkm->sm", pair_hot, pair_grad, preferred_element_type=F32).astype(BF)
        grad_in = dispatch(send_grad)

        pre_gate, pre_up, act_mix = gate_and_up(expert_in, w_gate, w_up)
        expert_out = rows_from((act_mix,), (w_down,))
        expert_out, grad_in = lax.optimization_barrier((expert_out, grad_in))
        d_pre_gate, d_pre_up = gate_and_up_backward(grad_in, w_down, pre_gate, pre_up)

        ff = act_mix.shape[1]
        ret_rows = dispatch(expert_out)
        grad_down = reduce_grad((act_mix[:, : ff // 2], act_mix[:, ff // 2 :]), grad_in)
        grad_gate_up = reduce_grad((d_pre_gate, d_pre_up), expert_in)
        d_expert_in = rows_from((d_pre_gate, d_pre_up), (w_gate, w_up))
        ret_rows, d_expert_in = lax.optimization_barrier((ret_rows, d_expert_in))
        d_rows = dispatch(d_expert_in)
        grad_down = to_owner_core(grad_down)
        grad_gate_up = to_owner_core(grad_gate_up)
        full_down = copy_out(gather_grad(grad_down))
        gate_up = gather_grad(grad_gate_up)
        full_gate = jnp.swapaxes(gate_up[:, :ff], 1, 2)
        full_up = jnp.swapaxes(gate_up[:, ff:], 1, 2)

        pair_out = jnp.dot(pair_hot.reshape(tokens_dev * n_top, slots), ret_rows, preferred_element_type=F32).reshape(tokens_dev, n_top, model_dim)
        mixed = jnp.sum(gate_probs[..., None] * pair_out, axis=1)
        moe_out = (x_f + mixed).astype(BF)
        d_logits = router_backward(gate_probs, pick_mask, pair_out, dout_f)
        d_hidden_moe = jnp.einsum("ts,sm->tm", token_hot, d_rows, preferred_element_type=F32)
        d_hidden_router = jnp.einsum("te,me->tm", d_logits, w_router, preferred_element_type=F32)
        d_hidden = (d_hidden_moe + d_hidden_router).astype(BF).astype(F32)
        grad_x = (dout_f + norm_backward(d_hidden, normed, inv_std, ln_gain)).astype(BF)
        small = small_psum([jnp.dot(lax.optimization_barrier(d_logits.T), hidden, preferred_element_type=F32), jnp.sum(d_hidden * normed, axis=0)[None], jnp.sum(d_hidden, axis=0)[None]])
        return (moe_out, grad_x, small[experts], small[experts + 1], small[:experts].T, full_gate, full_up, full_down)

    return jax.shard_map(local_step, mesh=inner, in_specs=(tok_spec, P(None), P(None), P(None, None), exp_spec, exp_spec, exp_spec, tok_spec, tok_spec, tok_spec), out_specs=(tok_spec, tok_spec, P(None), P(None), P(None, None), exp_spec, exp_spec, exp_spec), check_vma=False)
```
